32 devices in a mesh: dp: 8 (over z, x), seq: 4 (over y, core).
Axes of the slice: x: 2, y: 2, z: 4, core: 2. Of those that a mesh axis runs over, the one named last changes fastest.
Arguments:
- tokens: bfloat16 [4608, 3584], P('dp'), may hold values from -6 to 6
- positions: int32 [3, 4608], P(None, 'dp'), may hold values from 0 to 2047
- loss_mask: int32 [4608], P('dp'), may hold values from 0 to 1, as said below
- sample_tokens: int32 [8, 3], replicated, may hold values from 96 to 384, as said below
- dest_slot: int32 [4608], P('dp'), may hold values from 0 to 6143, as said below
- norm_gain: float32 [3584], replicated, may hold values from 0.5 to 1.5
- q_weight: bfloat16 [3584, 2048], P(None, 'seq'), may hold values from -0.09375 to 0.09375
- k_weight: bfloat16 [3584, 512], P(None, 'seq'), may hold values from -0.09375 to 0.09375
- v_weight: bfloat16 [3584, 512], P(None, 'seq'), may hold values from -0.09375 to 0.09375
- q_bias: float32 [2048], P('seq'), may hold values from -3 to 3
- k_bias: float32 [512], P('seq'), may hold values from -3 to 3
- v_bias: float32 [512], P('seq'), may hold values from -3 to 3
- o_weight: bfloat16 [2048, 3584], P('seq'), may hold values from -0.125 to 0.125
Outputs:
- mixed: bfloat16 [6144, 3584], P(('dp', 'seq'))
- token_weight: float32 [6144], P(('dp', 'seq'))
The draws below stay inside these ranges and needn't reach their ends.
Inputs may be any that keep to these rules, and one draw needn't show every extreme that they name: `sample_tokens`: row r gives the token counts of the samples in the buckets of receiver r, of 384, 192 and 192 slots; each count lies between half of its bucket's slots and all of them. Some receiver has all three buckets full. All counts together equal the number of rows of tokens. `dest_slot`: every row has a slot of its own, and the slots that rows take are exactly the first sample_tokens[r, b] slots of each bucket b of each receiver r. Of the rows of one sender at most 96 go to one receiver; a receiver whose buckets are all full takes exactly 96 rows from every sender. `loss_mask`: the first of each sender's 576 rows is 1.
All inputs are finite; a program needn't handle non-finite values.
Results may differ from the reference program's by a relative error of at most 0.015.
Values may be sent and summed in bfloat16 or wider, within the bound.
No kernel may reach another device: no remote copies, remote signals or barrier semaphores. Data moves between devices by JAX's collectives and lax.ppermute only.
A program may use at most 128 MiB of HBM per device.

```python
import math
import jax
import jax.numpy as jnp
from jax import lax

D = 3584
HQ = 16
KV = 4
DH = 128
BUCKET = 384
SRC = 576
N_DP = 8
N_SEQ = 4


def plan_tables(key):
    pairing_key = jax.random.fold_in(key, 11)
    length_key = jax.random.fold_in(key, 12)
    shuffle_key = jax.random.fold_in(key, 13)
    half_bucket = BUCKET // 2
    bucket_sizes = jnp.array([BUCKET, half_bucket, half_bucket], jnp.int32)
    pairing = jax.random.permutation(pairing_key, N_DP).astype(jnp.int32)
    pair_count = N_DP // 2
    first_lengths = jax.random.randint(length_key, (pair_count, 3), bucket_sizes // 2, bucket_sizes + 1).astype(jnp.int32)
    first_lengths = first_lengths.at[0].set(bucket_sizes)
    second_lengths = (3 * bucket_sizes // 2 - first_lengths).astype(jnp.int32)
    lengths = jnp.zeros((N_DP, 3), jnp.int32).at[pairing[0::2]].set(first_lengths).at[pairing[1::2]].set(second_lengths)
    local_slot = jnp.arange(2 * BUCKET, dtype=jnp.int32)
    bucket_id = (local_slot >= BUCKET).astype(jnp.int32) + (local_slot >= BUCKET + half_bucket).astype(jnp.int32)
    starts = jnp.array([0, BUCKET, BUCKET + half_bucket], jnp.int32)
    offset = local_slot - starts[bucket_id]
    filled = (offset[None, :] < lengths[:, bucket_id]).reshape(-1).astype(jnp.int32)
    order_index = (jnp.cumsum(filled) - 1).astype(jnp.int32)
    sender = order_index % N_DP
    within = jnp.clip(order_index // N_DP, 0, SRC - 1)
    sender_keys = jax.random.split(shuffle_key, N_DP)
    shuffles = jax.vmap(lambda one_key: jax.random.permutation(one_key, SRC))(sender_keys).astype(jnp.int32)
    source_row = (sender * SRC + shuffles[sender, within]).astype(jnp.int32)
    target = jnp.where(filled > 0, source_row, N_DP * SRC)
    global_slot = jnp.arange(N_DP * 2 * BUCKET, dtype=jnp.int32)
    dest = jnp.zeros((N_DP * SRC,), jnp.int32).at[target].set(global_slot, mode='drop')
    return (lengths, dest)


def draw_sample_tokens(key, part):
    return plan_tables(key)[0]


def draw_dest_slot(key, part):
    return plan_tables(key)[1]


def draw_loss_mask(key, part):
    row_total = N_DP * SRC
    row_ids = jnp.arange(row_total, dtype=jnp.int32)
    sender = row_ids // SRC
    level = jax.random.randint(jax.random.fold_in(key, 22), (), 15, 86).astype(jnp.int32)
    jitter = jax.random.randint(jax.random.fold_in(key, 23), (N_DP,), 50, 151).astype(jnp.int32)
    ramp = N_DP - 1 + 2 * sender
    threshold = level * ramp * jitter[sender]
    drawn = jax.random.randint(jax.random.fold_in(key, 21), (row_total,), 0, 100 * (3 * N_DP - 3) * 150)
    chosen = (drawn < threshold) | (row_ids % SRC == 0)
    return chosen.astype(jnp.int32)


def with_ends(values, key, low, high):
    dims = values.shape
    index_at = [jax.random.randint(jax.random.fold_in(key, axis), (), 0, dims[axis]) for axis in range(len(dims))]
    values = values.at[tuple(index_at)].set(low)
    longest = dims.index(max(dims))
    index_at[longest] = (index_at[longest] + 1) % dims[longest]
    return values.at[tuple(index_at)].set(high)


def block_levels(own_key, extent, shards, smallest, top_value):
    level, own = 1.0, jax.random.fold_in(own_key, 6)
    for position, parts in shards:
        draws = jnp.exp(jax.random.uniform(jax.random.fold_in(own, position), (parts,), jnp.float32, smallest / len(shards), top_value / len(shards)))
        level = level * jnp.repeat(draws, extent[position] // parts).reshape([-1 if axis == position else 1 for axis in range(len(extent))])
    return level


def bell_draw(own_key, shape, spread, bound, cuts=(), held_as=jnp.bfloat16):
    level = block_levels(own_key, shape, cuts, -0.22, 0.18) if cuts else 1.0
    entries = jax.random.normal(own_key, shape, jnp.float32) * spread * level
    return jnp.minimum(jnp.maximum(entries, -bound), bound).astype(held_as)


def setup_inputs(seed: int = 0) -> dict:
    streams_of = jax.random.split(jax.random.key(seed), 14)
    tokens = bell_draw(streams_of[0], (N_DP * SRC, D), 1.0, 6.0, ((0, 8),))
    positions = with_ends(jax.random.randint(streams_of[1], (3, N_DP * SRC), 0, 2048), jax.random.fold_in(streams_of[1], 1), 0, 2047).astype(jnp.int32)
    loss_mask = draw_loss_mask(jax.random.fold_in(streams_of[13], 71), 0)
    sample_tokens = draw_sample_tokens(jax.random.fold_in(streams_of[13], 71), 0)
    dest_slot = draw_dest_slot(jax.random.fold_in(streams_of[13], 71), 0)
    norm_gain = jnp.clip(1.0 + 0.1 * jax.random.normal(streams_of[5], (D,), jnp.float32), 0.5, 1.5)
    q_weight = bell_draw(streams_of[6], (D, HQ * DH), D ** -0.5, 0.09375, ((1, 4),))
    k_weight = bell_draw(streams_of[7], (D, KV * DH), D ** -0.5, 0.09375, ((1, 4),))
    v_weight = bell_draw(streams_of[8], (D, KV * DH), D ** -0.5, 0.09375, ((1, 4),))
    q_bias = bell_draw(streams_of[9], (HQ * DH,), 0.5, 3.0, ((0, 4),), jnp.float32)
    k_bias = bell_draw(streams_of[10], (KV * DH,), 0.5, 3.0, ((0, 4),), jnp.float32)
    v_bias = bell_draw(streams_of[11], (KV * DH,), 0.5, 3.0, ((0, 4),), jnp.float32)
    o_weight = bell_draw(streams_of[12], (HQ * DH, D), (HQ * DH) ** -0.5, 0.125, ((0, 4),))
    return {"tokens": tokens, "positions": positions, "loss_mask": loss_mask, "sample_tokens": sample_tokens, "dest_slot": dest_slot, "norm_gain": norm_gain, "q_weight": q_weight, "k_weight": k_weight, "v_weight": v_weight, "q_bias": q_bias, "k_bias": k_bias, "v_bias": v_bias, "o_weight": o_weight}


NORM_EPSILON = 1e-06
ROPE_BASE = 1000000.0

def rms_norm(rows_in, gain):
    widened = rows_in.astype(jnp.float32)
    mean_square = lax.optimization_barrier(jnp.mean(widened * widened, axis=-1, keepdims=True))
    return (widened * lax.rsqrt(mean_square + NORM_EPSILON) * gain).astype(jnp.bfloat16)

def rotary_tables(position_ids, head_size):
    half_size = head_size // 2
    pair_index = jnp.arange(half_size, dtype=jnp.int32)
    inv_freq = jnp.exp(pair_index.astype(jnp.float32) * (-2.0 * math.log(ROPE_BASE) / head_size))
    time_limit = head_size // 8
    height_limit = time_limit + 3 * head_size // 16
    chosen = jnp.where(pair_index[None, :] < time_limit, position_ids[0][:, None], jnp.where(pair_index[None, :] < height_limit, position_ids[1][:, None], position_ids[2][:, None]))
    angles = chosen.astype(jnp.float32) * inv_freq[None, :]
    return (jnp.cos(angles), jnp.sin(angles))

def rotate(heads_in, cosine, sine_part):
    half_size = heads_in.shape[-1] // 2
    first_half = heads_in[..., :half_size]
    second_half = heads_in[..., half_size:]
    cosine = cosine[:, None, :]
    sine_part = sine_part[:, None, :]
    return jnp.concatenate([first_half * cosine - second_half * sine_part, second_half * cosine + first_half * sine_part], axis=-1)

def attend_group(queries, key_rows, value_rows, lengths):
    block_count = queries.shape[0]
    row_count = queries.shape[1]
    scores = jnp.einsum('bqagd,bkad->bagqk', queries.astype(jnp.float32), key_rows.astype(jnp.float32)) * (1.0 / math.sqrt(DH))
    places = jnp.arange(row_count, dtype=jnp.int32)
    allowed = (places[:, None] >= places[None, :])[None] & (places[None, None, :] < lengths[:, None, None])
    scores = jnp.where(allowed[:, None, None], scores, -1e+30)
    weights = jax.nn.softmax(scores, axis=-1).astype(jnp.bfloat16)
    context = jnp.einsum('bagqk,bkad->bqagd', weights.astype(jnp.float32), value_rows.astype(jnp.float32))
    live_rows = places[None, :] < lengths[:, None]
    context = jnp.where(live_rows[:, :, None, None, None], context, 0.0).astype(jnp.bfloat16)
    return context.reshape(block_count * row_count, -1)

def attend_buckets(q_rows, k_rows, v_rows, lengths, kv_count, group_size):
    half_bucket = BUCKET // 2
    first_part = attend_group(q_rows[:BUCKET].reshape(1, BUCKET, kv_count, group_size, DH), k_rows[:BUCKET].reshape(1, BUCKET, kv_count, DH), v_rows[:BUCKET].reshape(1, BUCKET, kv_count, DH), lengths[:1])
    second_part = attend_group(q_rows[BUCKET:].reshape(2, half_bucket, kv_count, group_size, DH), k_rows[BUCKET:].reshape(2, half_bucket, kv_count, DH), v_rows[BUCKET:].reshape(2, half_bucket, kv_count, DH), lengths[1:])
    return jnp.concatenate([first_part, second_part], axis=0)

def reference(tokens, positions, loss_mask, sample_tokens, dest_slot, norm_gain, q_weight, k_weight, v_weight, q_bias, k_bias, v_bias, o_weight):
    peer_count = sample_tokens.shape[0]
    slot_count = 2 * BUCKET
    total_slots = peer_count * slot_count
    head_count = q_weight.shape[1] // DH
    kv_count = k_weight.shape[1] // DH
    group_size = head_count // kv_count
    normed = rms_norm(tokens, norm_gain)
    queries = (jnp.dot(normed, q_weight, preferred_element_type=jnp.float32) + q_bias).astype(jnp.bfloat16)
    key_rows = (jnp.dot(normed, k_weight, preferred_element_type=jnp.float32) + k_bias).astype(jnp.bfloat16)
    value_rows = (jnp.dot(normed, v_weight, preferred_element_type=jnp.float32) + v_bias).astype(jnp.bfloat16)
    cosine, sine_part = rotary_tables(positions, DH)
    queries = rotate(queries.astype(jnp.float32).reshape(-1, head_count, DH), cosine, sine_part).astype(jnp.bfloat16)
    key_rows = rotate(key_rows.astype(jnp.float32).reshape(-1, kv_count, DH), cosine, sine_part).astype(jnp.bfloat16)
    q_slots = jnp.zeros((total_slots, head_count * DH), jnp.bfloat16).at[dest_slot].set(queries.reshape(-1, head_count * DH))
    k_slots = jnp.zeros((total_slots, kv_count * DH), jnp.bfloat16).at[dest_slot].set(key_rows.reshape(-1, kv_count * DH))
    v_slots = jnp.zeros((total_slots, kv_count * DH), jnp.bfloat16).at[dest_slot].set(value_rows)

    def attend(inputs):
        q_rows, k_rows, v_rows, lengths = inputs
        return attend_buckets(q_rows, k_rows, v_rows, lengths, kv_count, group_size)
    context = lax.map(attend, (q_slots.reshape(peer_count, slot_count, head_count * DH), k_slots.reshape(peer_count, slot_count, kv_count * DH), v_slots.reshape(peer_count, slot_count, kv_count * DH), sample_tokens))
    context = context.reshape(total_slots, head_count * DH)
    slice_width = head_count * DH // N_SEQ
    head_total = jnp.zeros((total_slots, tokens.shape[1]), jnp.float32)
    for group_index in range(N_SEQ):
        partial_value = jnp.dot(context[:, group_index * slice_width:(group_index + 1) * slice_width], o_weight[group_index * slice_width:(group_index + 1) * slice_width], preferred_element_type=jnp.float32).astype(jnp.bfloat16)
        head_total = head_total + partial_value.astype(jnp.float32)
    mixed = head_total.astype(jnp.bfloat16)
    mask_float = loss_mask.astype(jnp.float32)
    token_count = jnp.sum(mask_float)
    row_scale = tokens.shape[0] / token_count
    token_weight = jnp.zeros((total_slots,), jnp.float32).at[dest_slot].set(mask_float * row_scale)
    return (mixed, token_weight)
```

```python
import math

import jax
import jax.numpy as jnp
from jax import lax
from jax.experimental import pallas as pl
from jax.experimental.pallas import tpu as pltpu
from jax.sharding import PartitionSpec as P

DH = 128
BUCKET = 384
NORM_EPSILON = 1e-06
ROPE_BASE = 1000000.0
META = 128
RADIX = 128


def rotary_tables(position_ids, head_size):
    half_size = head_size // 2
    lane = jnp.arange(head_size, dtype=jnp.int32)
    pair_index = lane % half_size
    inv_freq = jnp.exp(pair_index.astype(jnp.float32) * (-2.0 * math.log(ROPE_BASE) / head_size))
    time_limit = head_size // 8
    height_limit = time_limit + 3 * head_size // 16
    chosen = jnp.where(
        pair_index[None, :] < time_limit,
        position_ids[0][:, None],
        jnp.where(
            pair_index[None, :] < height_limit, position_ids[1][:, None], position_ids[2][:, None]
        ),
    )
    angles = chosen.astype(jnp.float32) * inv_freq[None, :]
    sign = jnp.where(lane < half_size, -1.0, 1.0)
    return jnp.cos(angles), jnp.sin(angles) * sign[None, :]


def chunk_of(width, limit):
    return max(c for c in range(128, limit + 1, 128) if width % c == 0)


def send_kernel(capacity, width, x_ref, gain_ref, wq_ref, wk_ref, wv_ref, bias_ref, cos_ref, sin_ref,
                peer_row_ref, peer_col_ref, meta_ref, out_ref, acc_ref, sq_ref, sel_ref):
    step = pl.program_id(0)
    rows = x_ref.shape[0]
    q_cols, k_cols = wq_ref.shape[1], wk_ref.shape[1]
    slots = out_ref.shape[0]

    @pl.when(step == 0)
    def _():
        acc_ref[...] = jnp.zeros_like(acc_ref)
        sq_ref[...] = jnp.zeros_like(sq_ref)
        peer_row = peer_row_ref[...]
        first = lax.broadcasted_iota(jnp.int32, (rows, rows), 0)
        second = lax.broadcasted_iota(jnp.int32, (rows, rows), 1)
        before = (peer_col_ref[...] == peer_row) & (first < second)
        ranking = jnp.sum(jnp.where(before, 1, 0), axis=0, keepdims=True)
        buffer_slot = peer_row * capacity + ranking
        place = lax.broadcasted_iota(jnp.int32, (slots, rows), 0)
        sel_ref[...] = jnp.where(place == buffer_slot, 1.0, 0.0).astype(jnp.bfloat16)

    wide = x_ref[...].astype(jnp.float32)
    square = wide * wide
    total = sq_ref[...]
    for c in range(0, wide.shape[1], 128):
        total = total + square[:, c : c + 128]
    sq_ref[...] = total
    scaled = (wide * gain_ref[...]).astype(jnp.bfloat16)
    acc_ref[:, :q_cols] += jnp.dot(scaled, wq_ref[...], preferred_element_type=jnp.float32)
    acc_ref[:, q_cols : q_cols + k_cols] += jnp.dot(
        scaled, wk_ref[...], preferred_element_type=jnp.float32
    )
    acc_ref[:, q_cols + k_cols :] += jnp.dot(
        scaled, wv_ref[...], preferred_element_type=jnp.float32
    )

    @pl.when(step == pl.num_programs(0) - 1)
    def _():
        mean_square = jnp.sum(sq_ref[...], axis=1, keepdims=True) * (1.0 / width)
        inverse = lax.rsqrt(mean_square + NORM_EPSILON)
        cosine, sine = cos_ref[...], sin_ref[...]
        pick = sel_ref[...]
        for c in range(0, acc_ref.shape[1], DH):
            head = acc_ref[:, c : c + DH] * inverse + bias_ref[:, c : c + DH]
            head = head.astype(jnp.bfloat16)
            if c < q_cols + k_cols:
                head = head.astype(jnp.float32)
                head = (head * cosine + pltpu.roll(head, DH // 2, 1) * sine).astype(jnp.bfloat16)
            acc_ref[:, c : c + DH] = head.astype(jnp.float32)
        every = acc_ref[...].astype(jnp.bfloat16)
        cols = acc_ref.shape[1]
        out_ref[:, :cols] = jnp.dot(pick, every, preferred_element_type=jnp.float32).astype(
            jnp.bfloat16
        )
        meta = meta_ref[...]
        moved = jnp.dot(pick, meta, preferred_element_type=jnp.float32)
        column_sum = jnp.sum(meta.astype(jnp.float32), axis=0, keepdims=True)
        high = jnp.floor(column_sum * (1.0 / RADIX))
        lane = lax.broadcasted_iota(jnp.int32, (1, META), 1)
        digits = jnp.where(lane == 3, high, jnp.where(lane == 4, column_sum - RADIX * high, 0.0))
        row = lax.broadcasted_iota(jnp.int32, (slots, META), 0)
        leads = row % capacity == 0
        moved = jnp.where(lane >= 3, jnp.where(leads, digits, 0.0), moved)
        out_ref[:, cols:] = moved.astype(jnp.bfloat16)


def attend_kernel(total_rows, kv_count, group_size, lengths_ref, recv_ref, out_ref, weight_ref,
                  place_ref):
    slots = recv_ref.shape[0]
    q_cols = kv_count * group_size * DH
    cols = q_cols + 2 * kv_count * DH
    meta = recv_ref[:, cols:]
    row = lax.broadcasted_iota(jnp.int32, (8, META), 0)
    lane = lax.broadcasted_iota(jnp.int32, (8, META), 1)
    high = ((row == 0) & (lane == 0)) | ((row == 2) & (lane == 3))
    low = ((row == 0) & (lane == 1)) | ((row == 1) & (lane == 2)) | ((row == 2) & (lane == 4))
    decode = jnp.where(high, float(RADIX), jnp.where(low, 1.0, 0.0)).astype(jnp.bfloat16)
    across = (((1,), (1,)), ((), ()))
    facts = lax.dot_general(decode, meta, across, preferred_element_type=jnp.float32)
    slot_row = facts[0:1].astype(jnp.int32) - 1
    place = lax.broadcasted_iota(jnp.int32, (slots, slots), 0)
    chosen = jnp.where(place == slot_row, 1.0, 0.0).astype(jnp.bfloat16)
    place_ref[...] = jnp.dot(
        chosen, recv_ref[:, :cols], preferred_element_type=jnp.float32
    ).astype(jnp.bfloat16)
    flags = lax.dot_general(
        facts.astype(jnp.bfloat16), chosen, across, preferred_element_type=jnp.float32
    )
    count = jnp.sum(facts[2:3], axis=1, keepdims=True)
    weight_ref[...] = flags[1:2] * (total_rows / count)
    block = BUCKET // 2
    for bucket, start, size in ((0, 0, BUCKET), (1, BUCKET, block), (2, BUCKET + block, block)):
        length = lengths_ref[bucket]
        for first in range(0, size, block):
            keys = first + block
            places = first + lax.broadcasted_iota(jnp.int32, (block, keys), 0)
            others = lax.broadcasted_iota(jnp.int32, (block, keys), 1)
            allowed = (places >= others) & (others < length)
            live = first + lax.broadcasted_iota(jnp.int32, (block, DH), 0) < length
            for g in range(kv_count):
                k_at = q_cols + g * DH
                v_at = k_at + kv_count * DH
                k_rows = place_ref[start : start + keys, k_at : k_at + DH]
                v_rows = place_ref[start : start + keys, v_at : v_at + DH]
                for h in range(g * group_size, (g + 1) * group_size):
                    own = slice(start + first, start + first + block)
                    head = slice(h * DH, (h + 1) * DH)
                    scores = lax.dot_general(
                        place_ref[own, head], k_rows, across, preferred_element_type=jnp.float32
                    ) * (1.0 / math.sqrt(DH))
                    scores = jnp.where(allowed, scores, -1e30)
                    top = jnp.max(scores, axis=1, keepdims=True)
                    grown = jnp.exp(scores - top)
                    share = 1.0 / jnp.sum(grown, axis=1, keepdims=True)
                    probs = (grown * share).astype(jnp.bfloat16)
                    context = jnp.dot(probs, v_rows, preferred_element_type=jnp.float32)
                    out_ref[own, head] = jnp.where(live, context, 0.0).astype(jnp.bfloat16)


def sum_groups(context, o_weight, seq_count, seq_index):
    def product(rows):
        return jnp.dot(rows, o_weight, preferred_element_type=jnp.float32).astype(jnp.bfloat16)

    if seq_count != 4:
        return lax.psum_scatter(product(context), "seq", scatter_dimension=0, tiled=True)
    near = [(i, i ^ 1) for i in range(seq_count)]
    far = [(i, i ^ 2) for i in range(seq_count)]
    parts = context.reshape(seq_count, -1, context.shape[1])

    def part(which):
        return lax.dynamic_index_in_dim(parts, which, 0, keepdims=False)

    def widened(array):
        return array.astype(jnp.float32)

    from_near = lax.ppermute(product(part(seq_index ^ 3)), "seq", near)
    for_far = product(part(seq_index ^ 2))
    from_far = lax.ppermute((widened(for_far) + widened(from_near)).astype(jnp.bfloat16), "seq", far)
    own_near = lax.ppermute(product(part(seq_index ^ 1)), "seq", near)
    own = product(part(seq_index))
    return (widened(own) + widened(own_near) + widened(from_far)).astype(jnp.bfloat16)


def per_device(tokens, positions, loss_mask, sample_tokens, dest_slot, norm_gain, q_weight, k_weight,
               v_weight, q_bias, k_bias, v_bias, o_weight):
    peer_count = lax.axis_size("dp")
    seq_count = lax.axis_size("seq")
    own_index = lax.axis_index("dp")
    seq_index = lax.axis_index("seq")
    rows, width = tokens.shape
    slots = 2 * BUCKET
    capacity = slots // peer_count
    q_cols, k_cols, v_cols = q_weight.shape[1], k_weight.shape[1], v_weight.shape[1]
    kv_count = k_cols // DH
    group_size = q_cols // k_cols
    cols = q_cols + k_cols + v_cols
    peer = dest_slot // slots
    code = dest_slot % slots + 1
    lane = jnp.arange(META, dtype=jnp.int32)[None, :]
    meta = jnp.where(
        lane == 0,
        (code // RADIX)[:, None],
        jnp.where(lane == 1, (code % RADIX)[:, None], jnp.where(lane < 5, loss_mask[:, None], 0)),
    ).astype(jnp.bfloat16)
    cosine, sine = rotary_tables(positions, DH)
    bias = jnp.concatenate([q_bias, k_bias, v_bias])[None, :]
    chunk = chunk_of(width, 512)
    whole = lambda *shape: pl.BlockSpec(shape, lambda i: (0, 0))
    down = lambda n: pl.BlockSpec((chunk, n), lambda i: (i, 0))
    across = lambda n: pl.BlockSpec((n, chunk), lambda i: (0, i))
    send = pl.pallas_call(
        lambda *refs: send_kernel(capacity, width, *refs),
        name="project_and_pack",
        grid=(width // chunk,),
        in_specs=[across(rows), across(1), down(q_cols), down(k_cols), down(v_cols), whole(1, cols),
                  whole(rows, DH), whole(rows, DH), whole(1, rows), whole(rows, 1),
                  whole(rows, META)],
        out_specs=whole(slots, cols + META),
        out_shape=jax.ShapeDtypeStruct((slots, cols + META), jnp.bfloat16),
        scratch_shapes=[pltpu.VMEM((rows, cols), jnp.float32), pltpu.VMEM((rows, 128), jnp.float32),
                        pltpu.VMEM((slots, rows), jnp.bfloat16)],
    )(tokens, norm_gain[None, :], q_weight, k_weight, v_weight, bias, cosine, sine, peer[None, :],
      peer[:, None], meta)
    recv = lax.all_to_all(
        send.reshape(peer_count, capacity, cols + META), "dp", split_axis=0, concat_axis=0, tiled=True
    ).reshape(slots, cols + META)
    lengths = sample_tokens[own_index]
    context, weights = pl.pallas_call(
        lambda *refs: attend_kernel(float(peer_count * rows), kv_count, group_size, *refs),
        name="place_and_attend",
        in_specs=[pl.BlockSpec(memory_space=pltpu.SMEM), pl.BlockSpec(memory_space=pltpu.VMEM)],
        out_specs=[pl.BlockSpec(memory_space=pltpu.VMEM), pl.BlockSpec(memory_space=pltpu.VMEM)],
        out_shape=[jax.ShapeDtypeStruct((slots, q_cols), jnp.bfloat16),
                   jax.ShapeDtypeStruct((1, slots), jnp.float32)],
        scratch_shapes=[pltpu.VMEM((slots, cols), jnp.bfloat16)],
    )(lengths, recv)
    part_rows = slots // seq_count
    own_weights = lax.dynamic_slice_in_dim(weights[0], seq_index * part_rows, part_rows, 0)
    return sum_groups(context, o_weight, seq_count, seq_index), own_weights


def solution(mesh):
    return jax.shard_map(
        per_device,
        mesh=mesh,
        in_specs=(P("dp", None), P(None, "dp"), P("dp"), P(), P("dp"), P(), P(None, "seq"),
                  P(None, "seq"), P(None, "seq"), P("seq"), P("seq"), P("seq"), P("seq", None)),
        out_specs=(P(("dp", "seq"), None), P(("dp", "seq"))),
        check_vma=False,
    )
```

```python
import math

import jax
import jax.numpy as jnp
from jax import lax
from jax.experimental import pallas as pl
from jax.experimental.pallas import tpu as pltpu
from jax.sharding import PartitionSpec as P

DH = 128
BUCKET = 384
NORM_EPSILON = 1e-06
ROPE_BASE = 1000000.0
META = 128
RADIX = 128


def chunk_of(width, limit):
    return max(c for c in range(128, limit + 1, 128) if width % c == 0)


def column_weights(count):
    row = lax.broadcasted_iota(jnp.int32, (count, DH), 0)
    lane = lax.broadcasted_iota(jnp.int32, (count, DH), 1)
    pair = lane % (DH // 2)
    time_limit = DH // 8
    height_limit = time_limit + 3 * DH // 16
    axis = jnp.where(pair < time_limit, 0, jnp.where(pair < height_limit, 1, 2))
    ids = jnp.where(row == 2 * axis, float(RADIX), jnp.where(row == 2 * axis + 1, 1.0, 0.0))
    carried = ((row == 6) & (lane == 0)) | ((row == 7) & (lane == 1))
    carried = carried | ((row == 8) & (lane >= 2) & (lane < 5))
    return ids, jnp.where(carried, 1.0, 0.0), jnp.where(row == 9, 1.0, 0.0)


def send_kernel(capacity, width, x_ref, gain_ref, wq_ref, wk_ref, wv_ref, bq_ref, bk_ref, bv_ref,
                info_ref, out_ref, acc_ref, sq_ref, sel_ref, cos_ref, sin_ref, meta_ref):
    step = pl.program_id(0)
    rows, chunk = x_ref.shape
    q_cols, k_cols = wq_ref.shape[1], wk_ref.shape[1]
    slots = out_ref.shape[0]

    @pl.when(step == 0)
    def _():
        acc_ref[...] = jnp.zeros_like(acc_ref)
        sq_ref[...] = jnp.zeros_like(sq_ref)
        info = info_ref[...]

        def columns(weights):
            return lax.dot_general(info, weights.astype(jnp.bfloat16), (((0,), (0,)), ((), ())),
                                   preferred_element_type=jnp.float32)

        ids, carried, peers = (columns(w) for w in column_weights(info.shape[0]))
        meta_ref[...] = carried.astype(jnp.bfloat16)
        lane = lax.broadcasted_iota(jnp.int32, (1, DH), 1)
        pair = (lane % (DH // 2)).astype(jnp.float32)
        angles = ids * jnp.exp(pair * (-2.0 * math.log(ROPE_BASE) / DH))
        cos_ref[...] = jnp.cos(angles)
        sin_ref[...] = jnp.sin(angles) * jnp.where(lane < DH // 2, -1.0, 1.0)
        peer_row = info[9:10].astype(jnp.float32)
        first = lax.broadcasted_iota(jnp.int32, (rows, rows), 0)
        second = lax.broadcasted_iota(jnp.int32, (rows, rows), 1)
        before = (peers[:, :1] == peer_row) & (first < second)
        ranking = jnp.sum(jnp.where(before, 1.0, 0.0), axis=0, keepdims=True)
        buffer_slot = (peer_row * capacity + ranking).astype(jnp.int32)
        place = lax.broadcasted_iota(jnp.int32, (slots, rows), 0)
        sel_ref[...] = jnp.where(place == buffer_slot, 1.0, 0.0).astype(jnp.bfloat16)

    total = sq_ref[...]
    pieces = []
    for c in range(chunk // 128):
        wide = x_ref[:, c * 128 : (c + 1) * 128].astype(jnp.float32)
        total = total + wide * wide
        gain = gain_ref[pl.ds(step * (chunk // 128) + c, 1), :]
        pieces.append((wide * gain).astype(jnp.bfloat16))
    sq_ref[...] = total
    scaled = jnp.concatenate(pieces, axis=1)
    acc_ref[:, :q_cols] += jnp.dot(scaled, wq_ref[...], preferred_element_type=jnp.float32)
    acc_ref[:, q_cols : q_cols + k_cols] += jnp.dot(
        scaled, wk_ref[...], preferred_element_type=jnp.float32
    )
    acc_ref[:, q_cols + k_cols :] += jnp.dot(
        scaled, wv_ref[...], preferred_element_type=jnp.float32
    )

    @pl.when(step == pl.num_programs(0) - 1)
    def _():
        mean_square = jnp.sum(sq_ref[...], axis=1, keepdims=True) * (1.0 / width)
        inverse = lax.rsqrt(mean_square + NORM_EPSILON)
        cosine, sine = cos_ref[...], sin_ref[...]
        pick = sel_ref[...]
        bias = [r[i : i + 1] for r in (bq_ref, bk_ref, bv_ref) for i in range(r.shape[0])]
        for c in range(0, acc_ref.shape[1], DH):
            head = acc_ref[:, c : c + DH] * inverse + bias[c // DH]
            head = head.astype(jnp.bfloat16)
            if c < q_cols + k_cols:
                head = head.astype(jnp.float32)
                head = (head * cosine + pltpu.roll(head, DH // 2, 1) * sine).astype(jnp.bfloat16)
            acc_ref[:, c : c + DH] = head.astype(jnp.float32)
        every = acc_ref[...].astype(jnp.bfloat16)
        cols = acc_ref.shape[1]
        out_ref[:, :cols] = jnp.dot(pick, every, preferred_element_type=jnp.float32).astype(
            jnp.bfloat16
        )
        meta = meta_ref[...]
        moved = jnp.dot(pick, meta, preferred_element_type=jnp.float32)
        column_sum = jnp.sum(meta.astype(jnp.float32), axis=0, keepdims=True)
        high = jnp.floor(column_sum * (1.0 / RADIX))
        lane = lax.broadcasted_iota(jnp.int32, (1, META), 1)
        digits = jnp.where(lane == 3, high, jnp.where(lane == 4, column_sum - RADIX * high, 0.0))
        row = lax.broadcasted_iota(jnp.int32, (slots, META), 0)
        leads = row % capacity == 0
        moved = jnp.where(lane >= 3, jnp.where(leads, digits, 0.0), moved)
        out_ref[:, cols:] = moved.astype(jnp.bfloat16)


def attend_kernel(total_rows, kv_count, group_size, lengths_ref, recv_ref, out_ref, weight_ref,
                  place_ref):
    slots = recv_ref.shape[0]
    q_cols = kv_count * group_size * DH
    cols = q_cols + 2 * kv_count * DH
    meta = recv_ref[:, cols:]
    row = lax.broadcasted_iota(jnp.int32, (8, META), 0)
    lane = lax.broadcasted_iota(jnp.int32, (8, META), 1)
    high = ((row == 0) & (lane == 0)) | ((row == 2) & (lane == 3))
    low = ((row == 0) & (lane == 1)) | ((row == 1) & (lane == 2)) | ((row == 2) & (lane == 4))
    decode = jnp.where(high, float(RADIX), jnp.where(low, 1.0, 0.0)).astype(jnp.bfloat16)
    across = (((1,), (1,)), ((), ()))
    facts = lax.dot_general(decode, meta, across, preferred_element_type=jnp.float32)
    slot_row = facts[0:1].astype(jnp.int32) - 1
    place = lax.broadcasted_iota(jnp.int32, (slots, slots), 0)
    chosen = jnp.where(place == slot_row, 1.0, 0.0).astype(jnp.bfloat16)
    place_ref[...] = jnp.dot(
        chosen, recv_ref[:, :cols], preferred_element_type=jnp.float32
    ).astype(jnp.bfloat16)
    flags = lax.dot_general(
        facts.astype(jnp.bfloat16), chosen, across, preferred_element_type=jnp.float32
    )
    count = jnp.sum(facts[2:3], axis=1, keepdims=True)
    weight_ref[...] = flags[1:2] * (total_rows / count)
    block = BUCKET // 2
    for bucket, start, size in ((0, 0, BUCKET), (1, BUCKET, block), (2, BUCKET + block, block)):
        length = lengths_ref[bucket]
        for first in range(0, size, block):
            keys = first + block
            places = first + lax.broadcasted_iota(jnp.int32, (block, keys), 0)
            others = lax.broadcasted_iota(jnp.int32, (block, keys), 1)
            allowed = (places >= others) & (others < length)
            live = first + lax.broadcasted_iota(jnp.int32, (block, DH), 0) < length
            for g in range(kv_count):
                k_at = q_cols + g * DH
                v_at = k_at + kv_count * DH
                k_rows = place_ref[start : start + keys, k_at : k_at + DH]
                v_rows = place_ref[start : start + keys, v_at : v_at + DH]
                for h in range(g * group_size, (g + 1) * group_size):
                    own = slice(start + first, start + first + block)
                    head = slice(h * DH, (h + 1) * DH)
                    scores = lax.dot_general(
                        place_ref[own, head], k_rows, across, preferred_element_type=jnp.float32
                    ) * (1.0 / math.sqrt(DH))
                    scores = jnp.where(allowed, scores, -1e30)
                    top = jnp.max(scores, axis=1, keepdims=True)
                    grown = jnp.exp(scores - top)
                    share = 1.0 / jnp.sum(grown, axis=1, keepdims=True)
                    probs = (grown * share).astype(jnp.bfloat16)
                    context = jnp.dot(probs, v_rows, preferred_element_type=jnp.float32)
                    out_ref[own, head] = jnp.where(live, context, 0.0).astype(jnp.bfloat16)


def early_columns(width):
    return width * 5 // 7 // 128 * 128


def partners(seq_count, bit):
    return [(i, i ^ bit) for i in range(seq_count)]


def product(rows, weight):
    return jnp.dot(rows, weight, preferred_element_type=jnp.float32)


def sum_groups(context, o_weight, far_weight, seq_count, seq_index):
    if seq_count != 4:
        partial = product(context, o_weight).astype(jnp.bfloat16)
        return lax.psum_scatter(partial, "seq", scatter_dimension=0, tiled=True)
    near, far = partners(seq_count, 1), partners(seq_count, 2)
    early = far_weight.shape[1]
    head_weight, tail_weight = o_weight[:, :early], o_weight[:, early:]
    parts = context.reshape(2, 2, -1, context.shape[1])
    half, core = seq_index // 2, seq_index % 2

    def halves(which):
        return lax.dynamic_index_in_dim(parts, which, 0, keepdims=False)

    def one(pair, which):
        return lax.dynamic_index_in_dim(pair, which, 0, keepdims=False)

    away, home = halves(1 - half), halves(half)
    far_context = lax.ppermute(away, "seq", far)
    from_near = lax.ppermute(
        product(one(away, 1 - core), tail_weight).astype(jnp.bfloat16), "seq", near
    )
    for_far = product(one(away, core), tail_weight) + from_near.astype(jnp.float32)
    from_far = lax.ppermute(for_far.astype(jnp.bfloat16), "seq", far)

    def head_sum(which):
        return product(one(home, which), head_weight) + product(
            one(far_context, which), far_weight
        )

    near_tail = lax.ppermute(
        product(one(home, 1 - core), tail_weight).astype(jnp.bfloat16), "seq", near
    )
    near_head = lax.ppermute(head_sum(1 - core).astype(jnp.bfloat16), "seq", near)
    own_tail = product(one(home, core), tail_weight)
    head = head_sum(core) + near_head.astype(jnp.float32)
    tail = own_tail + near_tail.astype(jnp.float32) + from_far.astype(jnp.float32)
    return jnp.concatenate([head.astype(jnp.bfloat16), tail.astype(jnp.bfloat16)], axis=1)


def per_device(tokens, positions, loss_mask, sample_tokens, dest_slot, norm_gain, q_weight, k_weight,
               v_weight, q_bias, k_bias, v_bias, o_weight):
    peer_count = lax.axis_size("dp")
    seq_count = lax.axis_size("seq")
    own_index = lax.axis_index("dp")
    seq_index = lax.axis_index("seq")
    rows, width = tokens.shape
    slots = 2 * BUCKET
    capacity = slots // peer_count
    q_cols, k_cols, v_cols = q_weight.shape[1], k_weight.shape[1], v_weight.shape[1]
    kv_count = k_cols // DH
    group_size = q_cols // k_cols
    cols = q_cols + k_cols + v_cols
    far_weight = None
    if seq_count == 4:
        far_weight = lax.ppermute(
            o_weight[:, : early_columns(o_weight.shape[1])], "seq", partners(seq_count, 2)
        )
    peer = dest_slot // slots
    code = dest_slot % slots + 1
    digits = [d for p in (positions[0], positions[1], positions[2], code)
              for d in (p // RADIX, p % RADIX)]
    info = jnp.stack(digits + [loss_mask, peer] + [jnp.zeros_like(peer)] * 6).astype(jnp.bfloat16)
    chunk = chunk_of(width, 512)
    whole = lambda *shape: pl.BlockSpec(shape, lambda i: (0, 0))
    down = lambda n: pl.BlockSpec((chunk, n), lambda i: (i, 0))
    across = lambda n: pl.BlockSpec((n, chunk), lambda i: (0, i))
    send = pl.pallas_call(
        lambda *refs: send_kernel(capacity, width, *refs),
        name="project_and_pack",
        grid=(width // chunk,),
        in_specs=[across(rows), whole(width // 128, 128), down(q_cols), down(k_cols), down(v_cols),
                  whole(q_cols // DH, DH), whole(k_cols // DH, DH), whole(v_cols // DH, DH),
                  whole(*info.shape)],
        out_specs=whole(slots, cols + META),
        out_shape=jax.ShapeDtypeStruct((slots, cols + META), jnp.bfloat16),
        scratch_shapes=[pltpu.VMEM((rows, cols), jnp.float32), pltpu.VMEM((rows, 128), jnp.float32),
                        pltpu.VMEM((slots, rows), jnp.bfloat16), pltpu.VMEM((rows, DH), jnp.float32),
                        pltpu.VMEM((rows, DH), jnp.float32), pltpu.VMEM((rows, META), jnp.bfloat16)],
    )(tokens, norm_gain.reshape(-1, 128), q_weight, k_weight, v_weight, q_bias.reshape(-1, DH),
      k_bias.reshape(-1, DH), v_bias.reshape(-1, DH), info)
    recv = lax.all_to_all(
        send.reshape(peer_count, capacity, cols + META), "dp", split_axis=0, concat_axis=0, tiled=True
    ).reshape(slots, cols + META)
    lengths = sample_tokens[own_index]
    context, weights = pl.pallas_call(
        lambda *refs: attend_kernel(float(peer_count * rows), kv_count, group_size, *refs),
        name="place_and_attend",
        in_specs=[pl.BlockSpec(memory_space=pltpu.SMEM), pl.BlockSpec(memory_space=pltpu.VMEM)],
        out_specs=[pl.BlockSpec(memory_space=pltpu.VMEM), pl.BlockSpec(memory_space=pltpu.VMEM)],
        out_shape=[jax.ShapeDtypeStruct((slots, q_cols), jnp.bfloat16),
                   jax.ShapeDtypeStruct((1, slots), jnp.float32)],
        scratch_shapes=[pltpu.VMEM((slots, cols), jnp.bfloat16)],
    )(lengths, recv)
    part_rows = slots // seq_count
    own_weights = lax.dynamic_slice_in_dim(weights[0], seq_index * part_rows, part_rows, 0)
    return sum_groups(context, o_weight, far_weight, seq_count, seq_index), own_weights


def solution(mesh):
    return jax.shard_map(
        per_device,
        mesh=mesh,
        in_specs=(P("dp", None), P(None, "dp"), P("dp"), P(), P("dp"), P(), P(None, "seq"),
                  P(None, "seq"), P(None, "seq"), P("seq"), P("seq"), P("seq"), P("seq", None)),
        out_specs=(P(("dp", "seq"), None), P(("dp", "seq"))),
        check_vma=False,
    )
```

```python
import math

import jax
import jax.numpy as jnp
from jax import lax
from jax.experimental import pallas as pl
from jax.experimental.pallas import tpu as pltpu
from jax.sharding import PartitionSpec as P

DH = 128
BUCKET = 384
NORM_EPSILON = 1e-06
ROPE_BASE = 1000000.0
META = 128
RADIX = 128


def chunk_of(width, limit):
    return max(c for c in range(128, limit + 1, 128) if width % c == 0)


def column_weights(count):
    row = lax.broadcasted_iota(jnp.int32, (count, DH), 0)
    lane = lax.broadcasted_iota(jnp.int32, (count, DH), 1)
    pair = lane % (DH // 2)
    time_limit = DH // 8
    height_limit = time_limit + 3 * DH // 16
    axis = jnp.where(pair < time_limit, 0, jnp.where(pair < height_limit, 1, 2))
    ids = jnp.where(row == 2 * axis, float(RADIX), jnp.where(row == 2 * axis + 1, 1.0, 0.0))
    carried = ((row == 6) & (lane == 0)) | ((row == 7) & (lane == 1))
    carried = carried | ((row == 8) & (lane >= 2) & (lane < 5))
    return ids, jnp.where(carried, 1.0, 0.0), jnp.where(row == 9, 1.0, 0.0)


def send_kernel(capacity, width, x_ref, gain_ref, wq_ref, wk_ref, wv_ref, bq_ref, bk_ref, bv_ref,
                pos_ref, mask_ref, dest_ref, out_ref, acc_ref, sq_ref, sel_ref, cos_ref, sin_ref,
                meta_ref, info_ref):
    step = pl.program_id(0)
    rows, chunk = x_ref.shape
    q_cols, k_cols = wq_ref.shape[1], wk_ref.shape[1]
    slots = out_ref.shape[0]

    @pl.when(step == 0)
    def _():
        acc_ref[...] = jnp.zeros_like(acc_ref)
        sq_ref[...] = jnp.zeros_like(sq_ref)
        dest = dest_ref[...].astype(jnp.float32)
        peer_row = jnp.floor((dest + 0.5) * (1.0 / slots))
        code = dest - peer_row * slots + 1.0
        info_ref[...] = jnp.zeros_like(info_ref)
        numbers = [pos_ref[i : i + 1].astype(jnp.float32) for i in range(3)] + [code]
        for i, number in enumerate(numbers):
            high = jnp.floor(number * (1.0 / RADIX))
            info_ref[2 * i : 2 * i + 1] = high
            info_ref[2 * i + 1 : 2 * i + 2] = number - RADIX * high
        info_ref[8:9] = mask_ref[...].astype(jnp.float32)
        info_ref[9:10] = peer_row
        info = info_ref[...].astype(jnp.bfloat16)

        def columns(weights):
            return lax.dot_general(info, weights.astype(jnp.bfloat16), (((0,), (0,)), ((), ())),
                                   preferred_element_type=jnp.float32)

        ids, carried, peers = (columns(w) for w in column_weights(info.shape[0]))
        meta_ref[...] = carried.astype(jnp.bfloat16)
        lane = lax.broadcasted_iota(jnp.int32, (1, DH), 1)
        pair = (lane % (DH // 2)).astype(jnp.float32)
        angles = ids * jnp.exp(pair * (-2.0 * math.log(ROPE_BASE) / DH))
        cos_ref[...] = jnp.cos(angles)
        sin_ref[...] = jnp.sin(angles) * jnp.where(lane < DH // 2, -1.0, 1.0)
        first = lax.broadcasted_iota(jnp.int32, (rows, rows), 0)
        second = lax.broadcasted_iota(jnp.int32, (rows, rows), 1)
        before = (peers[:, :1] == peer_row) & (first < second)
        ranking = jnp.sum(jnp.where(before, 1.0, 0.0), axis=0, keepdims=True)
        buffer_slot = (peer_row * capacity + ranking).astype(jnp.int32)
        place = lax.broadcasted_iota(jnp.int32, (slots, rows), 0)
        sel_ref[...] = jnp.where(place == buffer_slot, 1.0, 0.0).astype(jnp.bfloat16)

    total = sq_ref[...]
    pieces = []
    for c in range(chunk // 128):
        wide = x_ref[:, c * 128 : (c + 1) * 128].astype(jnp.float32)
        total = total + wide * wide
        gain = gain_ref[pl.ds(step * (chunk // 128) + c, 1), :]
        pieces.append((wide * gain).astype(jnp.bfloat16))
    sq_ref[...] = total
    scaled = jnp.concatenate(pieces, axis=1)
    acc_ref[:, :q_cols] += jnp.dot(scaled, wq_ref[...], preferred_element_type=jnp.float32)
    acc_ref[:, q_cols : q_cols + k_cols] += jnp.dot(
        scaled, wk_ref[...], preferred_element_type=jnp.float32
    )
    acc_ref[:, q_cols + k_cols :] += jnp.dot(
        scaled, wv_ref[...], preferred_element_type=jnp.float32
    )

    @pl.when(step == pl.num_programs(0) - 1)
    def _():
        mean_square = jnp.sum(sq_ref[...], axis=1, keepdims=True) * (1.0 / width)
        inverse = lax.rsqrt(mean_square + NORM_EPSILON)
        cosine, sine = cos_ref[...], sin_ref[...]
        pick = sel_ref[...]
        bias = [r[i : i + 1] for r in (bq_ref, bk_ref, bv_ref) for i in range(r.shape[0])]
        for c in range(0, acc_ref.shape[1], DH):
            head = acc_ref[:, c : c + DH] * inverse + bias[c // DH]
            head = head.astype(jnp.bfloat16)
            if c < q_cols + k_cols:
                head = head.astype(jnp.float32)
                head = (head * cosine + pltpu.roll(head, DH // 2, 1) * sine).astype(jnp.bfloat16)
            acc_ref[:, c : c + DH] = head.astype(jnp.float32)
        every = acc_ref[...].astype(jnp.bfloat16)
        cols = acc_ref.shape[1]
        out_ref[:, :cols] = jnp.dot(pick, every, preferred_element_type=jnp.float32).astype(
            jnp.bfloat16
        )
        meta = meta_ref[...]
        moved = jnp.dot(pick, meta, preferred_element_type=jnp.float32)
        column_sum = jnp.sum(meta.astype(jnp.float32), axis=0, keepdims=True)
        high = jnp.floor(column_sum * (1.0 / RADIX))
        lane = lax.broadcasted_iota(jnp.int32, (1, META), 1)
        digits = jnp.where(lane == 3, high, jnp.where(lane == 4, column_sum - RADIX * high, 0.0))
        row = lax.broadcasted_iota(jnp.int32, (slots, META), 0)
        leads = row % capacity == 0
        moved = jnp.where(lane >= 3, jnp.where(leads, digits, 0.0), moved)
        out_ref[:, cols:] = moved.astype(jnp.bfloat16)


def attend_kernel(total_rows, kv_count, group_size, lengths_ref, recv_ref, out_ref, weight_ref,
                  place_ref):
    slots = recv_ref.shape[0]
    q_cols = kv_count * group_size * DH
    cols = q_cols + 2 * kv_count * DH
    meta = recv_ref[:, cols:]
    row = lax.broadcasted_iota(jnp.int32, (8, META), 0)
    lane = lax.broadcasted_iota(jnp.int32, (8, META), 1)
    high = ((row == 0) & (lane == 0)) | ((row == 2) & (lane == 3))
    low = ((row == 0) & (lane == 1)) | ((row == 1) & (lane == 2)) | ((row == 2) & (lane == 4))
    decode = jnp.where(high, float(RADIX), jnp.where(low, 1.0, 0.0)).astype(jnp.bfloat16)
    across = (((1,), (1,)), ((), ()))
    facts = lax.dot_general(decode, meta, across, preferred_element_type=jnp.float32)
    slot_row = facts[0:1].astype(jnp.int32) - 1
    place = lax.broadcasted_iota(jnp.int32, (slots, slots), 0)
    chosen = jnp.where(place == slot_row, 1.0, 0.0).astype(jnp.bfloat16)
    place_ref[...] = jnp.dot(
        chosen, recv_ref[:, :cols], preferred_element_type=jnp.float32
    ).astype(jnp.bfloat16)
    flags = lax.dot_general(
        facts.astype(jnp.bfloat16), chosen, across, preferred_element_type=jnp.float32
    )
    count = jnp.sum(facts[2:3], axis=1, keepdims=True)
    weight_ref[...] = flags[1:2] * (total_rows / count)
    block = BUCKET // 2
    for bucket, start, size in ((0, 0, BUCKET), (1, BUCKET, block), (2, BUCKET + block, block)):
        length = lengths_ref[bucket]
        for first in range(0, size, block):
            keys = first + block
            places = first + lax.broadcasted_iota(jnp.int32, (block, keys), 0)
            others = lax.broadcasted_iota(jnp.int32, (block, keys), 1)
            allowed = (places >= others) & (others < length)
            live = first + lax.broadcasted_iota(jnp.int32, (block, DH), 0) < length
            for g in range(kv_count):
                k_at = q_cols + g * DH
                v_at = k_at + kv_count * DH
                k_rows = place_ref[start : start + keys, k_at : k_at + DH]
                v_rows = place_ref[start : start + keys, v_at : v_at + DH]
                for h in range(g * group_size, (g + 1) * group_size):
                    own = slice(start + first, start + first + block)
                    head = slice(h * DH, (h + 1) * DH)
                    scores = lax.dot_general(
                        place_ref[own, head], k_rows, across, preferred_element_type=jnp.float32
                    ) * (1.0 / math.sqrt(DH))
                    scores = jnp.where(allowed, scores, -1e30)
                    top = jnp.max(scores, axis=1, keepdims=True)
                    grown = jnp.exp(scores - top)
                    share = 1.0 / jnp.sum(grown, axis=1, keepdims=True)
                    probs = (grown * share).astype(jnp.bfloat16)
                    context = jnp.dot(probs, v_rows, preferred_element_type=jnp.float32)
                    out_ref[own, head] = jnp.where(live, context, 0.0).astype(jnp.bfloat16)


def early_columns(width):
    first = width // 7 // 128 * 128
    return first, 4 * first


def partners(seq_count, bit):
    return [(i, i ^ bit) for i in range(seq_count)]


def product(rows, weight):
    return jnp.dot(rows, weight, preferred_element_type=jnp.float32)


def sum_groups(context, o_weight, far_weights, seq_count, seq_index):
    if seq_count != 4:
        partial = product(context, o_weight).astype(jnp.bfloat16)
        return lax.psum_scatter(partial, "seq", scatter_dimension=0, tiled=True)
    near, far = partners(seq_count, 1), partners(seq_count, 2)
    cuts = [0]
    for weight in far_weights:
        cuts.append(cuts[-1] + weight.shape[1])
    tail_weight = o_weight[:, cuts[-1] :]
    parts = context.reshape(2, 2, -1, context.shape[1])
    half, core = seq_index // 2, seq_index % 2

    def halves(which):
        return lax.dynamic_index_in_dim(parts, which, 0, keepdims=False)

    def one(pair, which):
        return lax.dynamic_index_in_dim(pair, which, 0, keepdims=False)

    away, home = halves(1 - half), halves(half)
    far_context = lax.ppermute(away, "seq", far)
    from_near = lax.ppermute(
        product(one(away, 1 - core), tail_weight).astype(jnp.bfloat16), "seq", near
    )
    for_far = product(one(away, core), tail_weight) + from_near.astype(jnp.float32)
    from_far = lax.ppermute(for_far.astype(jnp.bfloat16), "seq", far)

    def head_sum(which):
        return [
            product(one(home, which), o_weight[:, low:high]) + product(one(far_context, which), weight)
            for low, high, weight in zip(cuts, cuts[1:], far_weights)
        ]

    near_tail = lax.ppermute(
        product(one(home, 1 - core), tail_weight).astype(jnp.bfloat16), "seq", near
    )
    near_heads = [
        lax.ppermute(head.astype(jnp.bfloat16), "seq", near) for head in head_sum(1 - core)
    ]
    own_tail = product(one(home, core), tail_weight)
    heads = [head + got.astype(jnp.float32) for head, got in zip(head_sum(core), near_heads)]
    tail = own_tail + near_tail.astype(jnp.float32) + from_far.astype(jnp.float32)
    return jnp.concatenate([piece.astype(jnp.bfloat16) for piece in heads + [tail]], axis=1)


def per_device(tokens, positions, loss_mask, sample_tokens, dest_slot, norm_gain, q_weight, k_weight,
               v_weight, q_bias, k_bias, v_bias, o_weight):
    peer_count = lax.axis_size("dp")
    seq_count = lax.axis_size("seq")
    own_index = lax.axis_index("dp")
    seq_index = lax.axis_index("seq")
    rows, width = tokens.shape
    slots = 2 * BUCKET
    capacity = slots // peer_count
    q_cols, k_cols, v_cols = q_weight.shape[1], k_weight.shape[1], v_weight.shape[1]
    kv_count = k_cols // DH
    group_size = q_cols // k_cols
    cols = q_cols + k_cols + v_cols
    chunk = chunk_of(width, 512)
    whole = lambda *shape: pl.BlockSpec(shape, lambda i: (0, 0))
    down = lambda n: pl.BlockSpec((chunk, n), lambda i: (i, 0))
    across = lambda n: pl.BlockSpec((n, chunk), lambda i: (0, i))
    send = pl.pallas_call(
        lambda *refs: send_kernel(capacity, width, *refs),
        name="project_and_pack",
        grid=(width // chunk,),
        in_specs=[across(rows), whole(width // 128, 128), down(q_cols), down(k_cols), down(v_cols),
                  whole(q_cols // DH, DH), whole(k_cols // DH, DH), whole(v_cols // DH, DH),
                  whole(3, rows), whole(1, rows), whole(1, rows)],
        out_specs=whole(slots, cols + META),
        out_shape=jax.ShapeDtypeStruct((slots, cols + META), jnp.bfloat16),
        scratch_shapes=[pltpu.VMEM((rows, cols), jnp.float32), pltpu.VMEM((rows, 128), jnp.float32),
                        pltpu.VMEM((slots, rows), jnp.bfloat16), pltpu.VMEM((rows, DH), jnp.float32),
                        pltpu.VMEM((rows, DH), jnp.float32), pltpu.VMEM((rows, META), jnp.bfloat16),
                        pltpu.VMEM((16, rows), jnp.float32)],
    )(tokens, norm_gain.reshape(-1, 128), q_weight, k_weight, v_weight, q_bias.reshape(-1, DH),
      k_bias.reshape(-1, DH), v_bias.reshape(-1, DH), positions,
      loss_mask[None, :], dest_slot[None, :])
    far_weights = ()
    if seq_count == 4:
        first, early = early_columns(o_weight.shape[1])
        far = partners(seq_count, 2)
        far_first = lax.ppermute(o_weight[:, :first], "seq", far)
        send, far_first, later = lax.optimization_barrier((send, far_first, o_weight))
        far_weights = (far_first, lax.ppermute(later[:, first:early], "seq", far))
    recv = lax.all_to_all(
        send.reshape(peer_count, capacity, cols + META), "dp", split_axis=0, concat_axis=0, tiled=True
    ).reshape(slots, cols + META)
    lengths = sample_tokens[own_index]
    context, weights = pl.pallas_call(
        lambda *refs: attend_kernel(float(peer_count * rows), kv_count, group_size, *refs),
        name="place_and_attend",
        in_specs=[pl.BlockSpec(memory_space=pltpu.SMEM), pl.BlockSpec(memory_space=pltpu.VMEM)],
        out_specs=[pl.BlockSpec(memory_space=pltpu.VMEM), pl.BlockSpec(memory_space=pltpu.VMEM)],
        out_shape=[jax.ShapeDtypeStruct((slots, q_cols), jnp.bfloat16),
                   jax.ShapeDtypeStruct((1, slots), jnp.float32)],
        scratch_shapes=[pltpu.VMEM((slots, cols), jnp.bfloat16)],
    )(lengths, recv)
    part_rows = slots // seq_count
    own_weights = lax.dynamic_slice_in_dim(weights[0], seq_index * part_rows, part_rows, 0)
    return sum_groups(context, o_weight, far_weights, seq_count, seq_index), own_weights


def solution(mesh):
    return jax.shard_map(
        per_device,
        mesh=mesh,
        in_specs=(P("dp", None), P(None, "dp"), P("dp"), P(), P("dp"), P(), P(None, "seq"),
                  P(None, "seq"), P(None, "seq"), P("seq"), P("seq"), P("seq"), P("seq", None)),
        out_specs=(P(("dp", "seq"), None), P(("dp", "seq"))),
        check_vma=False,
    )
```

```python
import math

import jax
import jax.numpy as jnp
from jax import lax
from jax.experimental import pallas as pl
from jax.experimental.pallas import tpu as pltpu
from jax.sharding import PartitionSpec as P

DH = 128
BUCKET = 384
NORM_EPSILON = 1e-06
ROPE_BASE = 1000000.0
META = 128
RADIX = 128


def chunk_of(width, limit):
    return max(c for c in range(128, limit + 1, 128) if width % c == 0)


def column_weights(count):
    row = lax.broadcasted_iota(jnp.int32, (count, DH), 0)
    lane = lax.broadcasted_iota(jnp.int32, (count, DH), 1)
    pair = lane % (DH // 2)
    time_limit = DH // 8
    height_limit = time_limit + 3 * DH // 16
    axis = jnp.where(pair < time_limit, 0, jnp.where(pair < height_limit, 1, 2))
    ids = jnp.where(row == 2 * axis, float(RADIX), jnp.where(row == 2 * axis + 1, 1.0, 0.0))
    carried = ((row == 6) & (lane == 0)) | ((row == 7) & (lane == 1))
    carried = carried | ((row == 8) & (lane >= 2) & (lane < 5))
    return ids, jnp.where(carried, 1.0, 0.0), jnp.where(row == 9, 1.0, 0.0)


def send_kernel(capacity, width, x_ref, gain_ref, wq_ref, wk_ref, wv_ref, bq_ref, bk_ref, bv_ref,
                pos_ref, mask_ref, dest_ref, out_ref, acc_ref, sq_ref, sel_ref, cos_ref, sin_ref,
                meta_ref, info_ref):
    step = pl.program_id(0)
    rows, chunk = x_ref.shape
    q_cols, k_cols = wq_ref.shape[1], wk_ref.shape[1]
    slots = out_ref.shape[0]

    @pl.when(step == 0)
    def _():
        acc_ref[...] = jnp.zeros_like(acc_ref)
        sq_ref[...] = jnp.zeros_like(sq_ref)
        dest = dest_ref[...].astype(jnp.float32)
        peer_row = jnp.floor((dest + 0.5) * (1.0 / slots))
        code = dest - peer_row * slots + 1.0
        info_ref[...] = jnp.zeros_like(info_ref)
        numbers = [pos_ref[i : i + 1].astype(jnp.float32) for i in range(3)] + [code]
        for i, number in enumerate(numbers):
            high = jnp.floor(number * (1.0 / RADIX))
            info_ref[2 * i : 2 * i + 1] = high
            info_ref[2 * i + 1 : 2 * i + 2] = number - RADIX * high
        info_ref[8:9] = mask_ref[...].astype(jnp.float32)
        info_ref[9:10] = peer_row
        info = info_ref[...].astype(jnp.bfloat16)

        def columns(weights):
            return lax.dot_general(info, weights.astype(jnp.bfloat16), (((0,), (0,)), ((), ())),
                                   preferred_element_type=jnp.float32)

        ids, carried, peers = (columns(w) for w in column_weights(info.shape[0]))
        meta_ref[...] = carried.astype(jnp.bfloat16)
        lane = lax.broadcasted_iota(jnp.int32, (1, DH), 1)
        pair = (lane % (DH // 2)).astype(jnp.float32)
        angles = ids * jnp.exp(pair * (-2.0 * math.log(ROPE_BASE) / DH))
        cos_ref[...] = jnp.cos(angles)
        sin_ref[...] = jnp.sin(angles) * jnp.where(lane < DH // 2, -1.0, 1.0)
        first = lax.broadcasted_iota(jnp.int32, (rows, rows), 0)
        second = lax.broadcasted_iota(jnp.int32, (rows, rows), 1)
        before = (peers[:, :1] == peer_row) & (first < second)
        ranking = jnp.sum(jnp.where(before, 1.0, 0.0), axis=0, keepdims=True)
        buffer_slot = (peer_row * capacity + ranking).astype(jnp.int32)
        place = lax.broadcasted_iota(jnp.int32, (slots, rows), 0)
        sel_ref[...] = jnp.where(place == buffer_slot, 1.0, 0.0).astype(jnp.bfloat16)

    total = sq_ref[...]
    pieces = []
    for c in range(chunk // 128):
        wide = x_ref[:, c * 128 : (c + 1) * 128].astype(jnp.float32)
        total = total + wide * wide
        gain = gain_ref[pl.ds(step * (chunk // 128) + c, 1), :]
        pieces.append((wide * gain).astype(jnp.bfloat16))
    sq_ref[...] = total
    scaled = jnp.concatenate(pieces, axis=1)
    acc_ref[:, :q_cols] += jnp.dot(scaled, wq_ref[...], preferred_element_type=jnp.float32)
    acc_ref[:, q_cols : q_cols + k_cols] += jnp.dot(
        scaled, wk_ref[...], preferred_element_type=jnp.float32
    )
    acc_ref[:, q_cols + k_cols :] += jnp.dot(
        scaled, wv_ref[...], preferred_element_type=jnp.float32
    )

    @pl.when(step == pl.num_programs(0) - 1)
    def _():
        mean_square = jnp.sum(sq_ref[...], axis=1, keepdims=True) * (1.0 / width)
        inverse = lax.rsqrt(mean_square + NORM_EPSILON)
        cosine, sine = cos_ref[...], sin_ref[...]
        pick = sel_ref[...]
        bias = [r[i : i + 1] for r in (bq_ref, bk_ref, bv_ref) for i in range(r.shape[0])]
        for c in range(0, acc_ref.shape[1], DH):
            head = acc_ref[:, c : c + DH] * inverse + bias[c // DH]
            head = head.astype(jnp.bfloat16)
            if c < q_cols + k_cols:
                head = head.astype(jnp.float32)
                head = (head * cosine + pltpu.roll(head, DH // 2, 1) * sine).astype(jnp.bfloat16)
            acc_ref[:, c : c + DH] = head.astype(jnp.float32)
        every = acc_ref[...].astype(jnp.bfloat16)
        cols = acc_ref.shape[1]
        out_ref[:, :cols] = jnp.dot(pick, every, preferred_element_type=jnp.float32).astype(
            jnp.bfloat16
        )
        meta = meta_ref[...]
        moved = jnp.dot(pick, meta, preferred_element_type=jnp.float32)
        column_sum = jnp.sum(meta.astype(jnp.float32), axis=0, keepdims=True)
        high = jnp.floor(column_sum * (1.0 / RADIX))
        lane = lax.broadcasted_iota(jnp.int32, (1, META), 1)
        digits = jnp.where(lane == 3, high, jnp.where(lane == 4, column_sum - RADIX * high, 0.0))
        row = lax.broadcasted_iota(jnp.int32, (slots, META), 0)
        leads = row % capacity == 0
        moved = jnp.where(lane >= 3, jnp.where(leads, digits, 0.0), moved)
        out_ref[:, cols:] = moved.astype(jnp.bfloat16)


def attend_kernel(total_rows, kv_count, group_size, lengths_ref, recv_ref, out_ref, weight_ref,
                  place_ref):
    slots = recv_ref.shape[0]
    q_cols = kv_count * group_size * DH
    cols = q_cols + 2 * kv_count * DH
    meta = recv_ref[:, cols:]
    row = lax.broadcasted_iota(jnp.int32, (8, META), 0)
    lane = lax.broadcasted_iota(jnp.int32, (8, META), 1)
    high = ((row == 0) & (lane == 0)) | ((row == 2) & (lane == 3))
    low = ((row == 0) & (lane == 1)) | ((row == 1) & (lane == 2)) | ((row == 2) & (lane == 4))
    decode = jnp.where(high, float(RADIX), jnp.where(low, 1.0, 0.0)).astype(jnp.bfloat16)
    across = (((1,), (1,)), ((), ()))
    facts = lax.dot_general(decode, meta, across, preferred_element_type=jnp.float32)
    slot_row = facts[0:1].astype(jnp.int32) - 1
    place = lax.broadcasted_iota(jnp.int32, (slots, slots), 0)
    chosen = jnp.where(place == slot_row, 1.0, 0.0).astype(jnp.bfloat16)
    place_ref[...] = jnp.dot(
        chosen, recv_ref[:, :cols], preferred_element_type=jnp.float32
    ).astype(jnp.bfloat16)
    flags = lax.dot_general(
        facts.astype(jnp.bfloat16), chosen, across, preferred_element_type=jnp.float32
    )
    count = jnp.sum(facts[2:3], axis=1, keepdims=True)
    weight_ref[...] = flags[1:2] * (total_rows / count)
    block = BUCKET // 2
    for bucket, start, size in ((0, 0, BUCKET), (1, BUCKET, block), (2, BUCKET + block, block)):
        length = lengths_ref[bucket]
        for first in range(0, size, block):
            keys = first + block
            places = first + lax.broadcasted_iota(jnp.int32, (block, keys), 0)
            others = lax.broadcasted_iota(jnp.int32, (block, keys), 1)
            allowed = (places >= others) & (others < length)
            live = first + lax.broadcasted_iota(jnp.int32, (block, DH), 0) < length
            for g in range(kv_count):
                k_at = q_cols + g * DH
                v_at = k_at + kv_count * DH
                k_rows = place_ref[start : start + keys, k_at : k_at + DH]
                v_rows = place_ref[start : start + keys, v_at : v_at + DH]
                for h in range(g * group_size, (g + 1) * group_size):
                    own = slice(start + first, start + first + block)
                    head = slice(h * DH, (h + 1) * DH)
                    scores = lax.dot_general(
                        place_ref[own, head], k_rows, across, preferred_element_type=jnp.float32
                    ) * (1.0 / math.sqrt(DH))
                    scores = jnp.where(allowed, scores, -1e30)
                    top = jnp.max(scores, axis=1, keepdims=True)
                    grown = jnp.exp(scores - top)
                    share = 1.0 / jnp.sum(grown, axis=1, keepdims=True)
                    probs = (grown * share).astype(jnp.bfloat16)
                    context = jnp.dot(probs, v_rows, preferred_element_type=jnp.float32)
                    out_ref[own, head] = jnp.where(live, context, 0.0).astype(jnp.bfloat16)


def early_columns(width):
    first = width // 7 // 128 * 128
    return first, 4 * first


def partners(seq_count, bit):
    return [(i, i ^ bit) for i in range(seq_count)]


def product(rows, weight):
    return jnp.dot(rows, weight, preferred_element_type=jnp.float32)


def sum_groups(context, o_weight, far_weights, seq_count, seq_index):
    if seq_count != 4:
        partial = product(context, o_weight).astype(jnp.bfloat16)
        return lax.psum_scatter(partial, "seq", scatter_dimension=0, tiled=True)
    near, far = partners(seq_count, 1), partners(seq_count, 2)
    cuts = [0]
    for weight in far_weights:
        cuts.append(cuts[-1] + weight.shape[1])
    tail_weight = o_weight[:, cuts[-1] :]
    parts = context.reshape(2, 2, -1, context.shape[1])
    half, core = seq_index // 2, seq_index % 2

    def halves(which):
        return lax.dynamic_index_in_dim(parts, which, 0, keepdims=False)

    def one(pair, which):
        return lax.dynamic_index_in_dim(pair, which, 0, keepdims=False)

    away, home = halves(1 - half), halves(half)
    far_context = lax.ppermute(away, "seq", far)
    from_near = lax.ppermute(
        product(one(away, 1 - core), tail_weight).astype(jnp.bfloat16), "seq", near
    )
    for_far = product(one(away, core), tail_weight) + from_near.astype(jnp.float32)
    for_far, home = lax.optimization_barrier((for_far.astype(jnp.bfloat16), home))
    from_far = lax.ppermute(for_far, "seq", far)

    def head_sum(which):
        return [
            product(one(home, which), o_weight[:, low:high]) + product(one(far_context, which), weight)
            for low, high, weight in zip(cuts, cuts[1:], far_weights)
        ]

    near_tail = lax.ppermute(
        product(one(home, 1 - core), tail_weight).astype(jnp.bfloat16), "seq", near
    )
    near_heads = [
        lax.ppermute(head.astype(jnp.bfloat16), "seq", near) for head in head_sum(1 - core)
    ]
    own_tail = product(one(home, core), tail_weight)
    heads = [head + got.astype(jnp.float32) for head, got in zip(head_sum(core), near_heads)]
    tail = own_tail + near_tail.astype(jnp.float32) + from_far.astype(jnp.float32)
    return jnp.concatenate([piece.astype(jnp.bfloat16) for piece in heads + [tail]], axis=1)


def per_device(tokens, positions, loss_mask, sample_tokens, dest_slot, norm_gain, q_weight, k_weight,
               v_weight, q_bias, k_bias, v_bias, o_weight):
    peer_count = lax.axis_size("dp")
    seq_count = lax.axis_size("seq")
    own_index = lax.axis_index("dp")
    seq_index = lax.axis_index("seq")
    rows, width = tokens.shape
    slots = 2 * BUCKET
    capacity = slots // peer_count
    q_cols, k_cols, v_cols = q_weight.shape[1], k_weight.shape[1], v_weight.shape[1]
    kv_count = k_cols // DH
    group_size = q_cols // k_cols
    cols = q_cols + k_cols + v_cols
    chunk = chunk_of(width, 512)
    whole = lambda *shape: pl.BlockSpec(shape, lambda i: (0, 0))
    down = lambda n: pl.BlockSpec((chunk, n), lambda i: (i, 0))
    across = lambda n: pl.BlockSpec((n, chunk), lambda i: (0, i))
    send = pl.pallas_call(
        lambda *refs: send_kernel(capacity, width, *refs),
        name="project_and_pack",
        grid=(width // chunk,),
        in_specs=[across(rows), whole(width // 128, 128), down(q_cols), down(k_cols), down(v_cols),
                  whole(q_cols // DH, DH), whole(k_cols // DH, DH), whole(v_cols // DH, DH),
                  whole(3, rows), whole(1, rows), whole(1, rows)],
        out_specs=whole(slots, cols + META),
        out_shape=jax.ShapeDtypeStruct((slots, cols + META), jnp.bfloat16),
        scratch_shapes=[pltpu.VMEM((rows, cols), jnp.float32), pltpu.VMEM((rows, 128), jnp.float32),
                        pltpu.VMEM((slots, rows), jnp.bfloat16), pltpu.VMEM((rows, DH), jnp.float32),
                        pltpu.VMEM((rows, DH), jnp.float32), pltpu.VMEM((rows, META), jnp.bfloat16),
                        pltpu.VMEM((16, rows), jnp.float32)],
    )(tokens, norm_gain.reshape(-1, 128), q_weight, k_weight, v_weight, q_bias.reshape(-1, DH),
      k_bias.reshape(-1, DH), v_bias.reshape(-1, DH), positions,
      loss_mask[None, :], dest_slot[None, :])
    far_weights = ()
    if seq_count == 4:
        first, early = early_columns(o_weight.shape[1])
        far = partners(seq_count, 2)
        far_first = lax.ppermute(o_weight[:, :first], "seq", far)
        send, far_first, later = lax.optimization_barrier((send, far_first, o_weight))
        far_weights = (far_first, lax.ppermute(later[:, first:early], "seq", far))
    recv = lax.all_to_all(
        send.reshape(peer_count, capacity, cols + META), "dp", split_axis=0, concat_axis=0, tiled=True
    ).reshape(slots, cols + META)
    lengths = sample_tokens[own_index]
    context, weights = pl.pallas_call(
        lambda *refs: attend_kernel(float(peer_count * rows), kv_count, group_size, *refs),
        name="place_and_attend",
        in_specs=[pl.BlockSpec(memory_space=pltpu.SMEM), pl.BlockSpec(memory_space=pltpu.VMEM)],
        out_specs=[pl.BlockSpec(memory_space=pltpu.VMEM), pl.BlockSpec(memory_space=pltpu.VMEM)],
        out_shape=[jax.ShapeDtypeStruct((slots, q_cols), jnp.bfloat16),
                   jax.ShapeDtypeStruct((1, slots), jnp.float32)],
        scratch_shapes=[pltpu.VMEM((slots, cols), jnp.bfloat16)],
    )(lengths, recv)
    part_rows = slots // seq_count
    own_weights = lax.dynamic_slice_in_dim(weights[0], seq_index * part_rows, part_rows, 0)
    return sum_groups(context, o_weight, far_weights, seq_count, seq_index), own_weights


def solution(mesh):
    return jax.shard_map(
        per_device,
        mesh=mesh,
        in_specs=(P("dp", None), P(None, "dp"), P("dp"), P(), P("dp"), P(), P(None, "seq"),
                  P(None, "seq"), P(None, "seq"), P("seq"), P("seq"), P("seq"), P("seq", None)),
        out_specs=(P(("dp", "seq"), None), P(("dp", "seq"))),
        check_vma=False,
    )
```
